32 devices in a mesh: seq: 2 (over core), heads: 4 (over y, x), batch: 4 (over z).
Axes of the slice: x: 2, y: 2, z: 4, core: 2. Of those that a mesh axis runs over, the one named last changes fastest.
Arguments:
- queries: bfloat16 [4, 512, 8192], P('batch', 'seq', 'heads'), may hold values from -160 to 160
- keys: bfloat16 [4, 512, 1024], P('batch', 'seq', 'heads'), may hold values from -7 to 7
- values: bfloat16 [4, 512, 1024], P('batch', 'seq', 'heads'), may hold values from -6 to 6
- doc_lengths: int32 [4, 16], P('batch'), may hold values from 1 to 384, 512 in all within a row
- out_weight: bfloat16 [8192, 8192], P('heads', 'batch'), may hold values from -0.0625 to 0.0625
Outputs:
- projected: bfloat16 [4, 512, 8192], P('heads', 'seq', 'batch')
The draws below stay inside these ranges and needn't reach their ends.
Inputs may be any that keep to these rules, and one draw needn't show every extreme that they name: `doc_lengths`: each row sums to 512; no document is longer than 384 tokens and one is exactly 384.
All inputs are finite; a program needn't handle non-finite values.
Results may differ from the reference program's by a relative error of at most 0.012.
Values may be sent and summed in bfloat16 or wider, within the bound.
A program may use at most 64 MiB of HBM per device.

```python
import math
import jax
import jax.numpy as jnp
import numpy as np
from jax import lax

QUERY_HEAD_COUNT = 64
VALUE_KEY_HEADS = 8
HEAD_WIDTH = 128
D = 8192
DOCS = 16
QBLOCK = 128
PACKED_BATCH = 4
PACKED_LENGTH = 512
LONGEST = 384


def shared_keys(key):
    sampled_values = jax.random.normal(jax.random.fold_in(key, 11), (PACKED_BATCH, PACKED_LENGTH, VALUE_KEY_HEADS, HEAD_WIDTH), jnp.float32)
    sampled_values = jnp.clip(sampled_values, -6.0, 6.0)
    return sampled_values


def draw_keys(key, part):
    sampled_values = shared_keys(key)
    return sampled_values.reshape(PACKED_BATCH, PACKED_LENGTH, VALUE_KEY_HEADS * HEAD_WIDTH).astype(jnp.bfloat16)


def draw_queries(key, part):
    sampled_values = jax.random.normal(jax.random.fold_in(key, 21), (PACKED_BATCH, PACKED_LENGTH, QUERY_HEAD_COUNT, HEAD_WIDTH), jnp.float32)
    sampled_values = jnp.clip(sampled_values, -6.0, 6.0)
    return sampled_values.reshape(PACKED_BATCH, PACKED_LENGTH, QUERY_HEAD_COUNT * HEAD_WIDTH).astype(jnp.bfloat16)


def level_of(stream_key, dims, shards, low, top_value):
    def one(dim, blocks):
        draws = jax.random.uniform(jax.random.fold_in(jax.random.fold_in(stream_key, 6), dim), (blocks,), jnp.float32, low / len(shards), top_value / len(shards))
        return jnp.repeat(jnp.exp(draws), dims[dim] // blocks).reshape((-1,) + (1,) * (len(dims) - dim - 1))

    loudness = one(*shards[0])
    for cut in shards[1:]:
        loudness = loudness * one(*cut)
    return loudness


def length_profile(count, total, limit, lean):
    portions = [(1 << 20) // math.isqrt(grade ** lean) + 1 for grade in range(2, count + 1)]
    rest, given = total - limit - (count - 1), [1] * (count - 1)
    while rest > 0:
        candidates = [i for i in range(count - 1) if given[i] < limit]
        whole, budget = sum([portions[i] for i in candidates]), rest
        for i in candidates:
            more = min(limit - given[i], max(1, budget * portions[i] // whole), rest)
            given[i] = given[i] + more
            rest = rest - more
    return np.array([limit] + given)


def ragged_sizes(key, count, total, bound, skew):
    if count == 2:
        one = jax.random.randint(key, (), max(1, total - bound), min(bound, total - 1) + 1)
        return jnp.stack([one, total - one])
    tallies = jnp.asarray(length_profile(count, total, bound, skew), jnp.int32)
    twos = (count - 1) // 2
    giver, receiver = tallies[1:1 + 2 * twos:2], tallies[2:2 + 2 * twos:2]
    margin = jnp.minimum(giver - 1, bound - receiver)
    shifted = jax.random.randint(jax.random.fold_in(key, 1), (twos,), 0, 1 << 20) % (margin + 1)
    tallies = tallies.at[1:1 + 2 * twos:2].set(giver - shifted).at[2:2 + 2 * twos:2].set(receiver + shifted)
    return tallies[jax.random.permutation(jax.random.fold_in(key, 2), count)]


def centred(own_key, dims, width, limit, pieces=(), held_as=jnp.bfloat16):
    entries = jax.random.normal(own_key, dims, jnp.float32) * width
    if len(pieces) > 0:
        entries = level_of(own_key, dims, pieces, -0.22, 0.18) * entries
    return jnp.clip(entries, min=-limit, max=limit).astype(held_as)


def setup_inputs(seed: int = 0) -> dict:
    arg_keys = jax.random.split(jax.random.key(seed), 6)
    queries = draw_queries(jax.random.fold_in(arg_keys[5], 71), 0)
    keys = draw_keys(jax.random.fold_in(arg_keys[5], 71), 0)
    values = centred(arg_keys[2], (PACKED_BATCH, PACKED_LENGTH, VALUE_KEY_HEADS * HEAD_WIDTH), 1.0, 6.0, ((0, 4), (1, 2), (2, 4)))
    doc_lengths = jax.vmap(lambda own: ragged_sizes(own, DOCS, PACKED_LENGTH, LONGEST, 2))(jax.random.split(arg_keys[3], PACKED_BATCH)).reshape((PACKED_BATCH, DOCS)).astype(jnp.int32)
    out_weight = centred(arg_keys[4], (QUERY_HEAD_COUNT * HEAD_WIDTH, D), (QUERY_HEAD_COUNT * HEAD_WIDTH) ** -0.5, 0.0625, ((0, 4), (1, 4)))
    return dict(queries=queries, keys=keys, values=values, doc_lengths=doc_lengths, out_weight=out_weight)


def document_of(lengths):
    doc_ends = jnp.cumsum(lengths)
    positions = jnp.arange(PACKED_LENGTH, dtype=jnp.int32)
    return jnp.sum((positions[:, None] >= doc_ends[None, :]).astype(jnp.int32), axis=1)


def attend_sequence(bundle):
    query_sequence, key_sequence, value_sequence, lengths = bundle
    group_width = QUERY_HEAD_COUNT // VALUE_KEY_HEADS
    key_span = min(LONGEST + QBLOCK, PACKED_LENGTH)
    doc_ids = document_of(lengths)
    query_head_rows = query_sequence.reshape(PACKED_LENGTH, VALUE_KEY_HEADS, group_width, HEAD_WIDTH)
    key_head_rows = key_sequence.reshape(PACKED_LENGTH, VALUE_KEY_HEADS, HEAD_WIDTH)
    value_head_rows = value_sequence.reshape(PACKED_LENGTH, VALUE_KEY_HEADS, HEAD_WIDTH)

    def one_block(block_index):
        q_start = (block_index * QBLOCK).astype(jnp.int32)
        k_start = jnp.clip(q_start + QBLOCK - key_span, 0, PACKED_LENGTH - key_span).astype(jnp.int32)
        q_block = lax.dynamic_slice_in_dim(query_head_rows, q_start, QBLOCK, 0).astype(jnp.float32)
        k_block = lax.dynamic_slice_in_dim(key_head_rows, k_start, key_span, 0).astype(jnp.float32)
        v_block = lax.dynamic_slice_in_dim(value_head_rows, k_start, key_span, 0).astype(jnp.float32)
        scores = jnp.einsum("qhgd,khd->hgqk", q_block, k_block, precision=lax.Precision.HIGHEST) * (HEAD_WIDTH ** -0.5)
        q_pos = q_start + jnp.arange(QBLOCK, dtype=jnp.int32)
        k_pos = k_start + jnp.arange(key_span, dtype=jnp.int32)
        q_doc = lax.dynamic_slice_in_dim(doc_ids, q_start, QBLOCK, 0)
        k_doc = lax.dynamic_slice_in_dim(doc_ids, k_start, key_span, 0)
        allowed = (q_doc[:, None] == k_doc[None, :]) & (k_pos[None, :] <= q_pos[:, None])
        scores = jnp.where(allowed, scores, -jnp.inf)
        highest = jnp.max(scores, axis=-1, keepdims=True)
        weights = jnp.exp(scores - highest)
        denominator = jnp.sum(weights, axis=-1)
        rounded = lax.optimization_barrier(weights.astype(jnp.bfloat16)).astype(jnp.float32)
        summed = jnp.einsum("hgqk,khd->qhgd", rounded, v_block, precision=lax.Precision.HIGHEST)
        result = summed / jnp.transpose(denominator, (2, 0, 1))[..., None]
        return result.reshape(QBLOCK, QUERY_HEAD_COUNT * HEAD_WIDTH).astype(jnp.bfloat16)

    outputs = lax.map(one_block, jnp.arange(PACKED_LENGTH // QBLOCK, dtype=jnp.int32))
    return outputs.reshape(PACKED_LENGTH, QUERY_HEAD_COUNT * HEAD_WIDTH)


def reference(queries, keys, values, doc_lengths, out_weight):
    attended = lax.map(attend_sequence, (queries, keys, values, doc_lengths))
    flat_rows = attended.reshape(PACKED_BATCH * PACKED_LENGTH, QUERY_HEAD_COUNT * HEAD_WIDTH).astype(jnp.float32)
    projected = jnp.dot(flat_rows, out_weight.astype(jnp.float32), precision=lax.Precision.HIGHEST)
    return projected.astype(jnp.bfloat16).reshape(PACKED_BATCH, PACKED_LENGTH, D)
```

```python
import functools
import math

import jax
import jax.numpy as jnp
from jax import lax
from jax.experimental import pallas as pl
from jax.experimental.pallas import tpu as pltpu
from jax.sharding import PartitionSpec as P

HEAD_WIDTH = 128
DOCS = 16
PIECES = 16
AHEAD = 4
LAG = 1
COLS = 512
MESH = pl.DeviceIdType.MESH


def delay(d):
    return jnp.maximum(d - 1, 0)


def kernel(
    sizes, q_hbm, k_hbm, v_hbm, len_hbm, w_hbm, out_ref,
    w_ref, queries, keys, vals, lens, gath, stage, incoming,
    w_sem, load_sem, kv_send, kv_recv, z_send, z_recv, c_send, c_recv,
):
    seqs, groups, n, reach = sizes
    shard_len, q_width = queries.shape
    kv_width = keys.shape[1]
    columns = w_ref.shape[1]
    kv_heads = kv_width // HEAD_WIDTH
    per_kv = q_width // kv_width
    rows = shard_len // PIECES
    blocks = columns // COLS
    own_keys = reach * shard_len

    me = lax.axis_index("seq")
    head = lax.axis_index("heads")
    b = lax.axis_index("batch")

    barrier = pltpu.get_barrier_semaphore()

    def greet(axis, index):
        pl.semaphore_signal(barrier, inc=1, device_id={axis: index}, device_id_type=MESH)

    expected = 0
    for d in range(1, reach + 1):
        for cond, index in ((me >= d, me - d), (me + d < seqs, me + d)):
            expected = expected + cond.astype(jnp.int32)
            pl.when(cond)(functools.partial(greet, "seq", index))
    for cond, index in ((b > 0, b - 1), (b < n - 1, b + 1)):
        expected = expected + cond.astype(jnp.int32)
        pl.when(cond)(functools.partial(greet, "batch", index))
    for d in range(1, groups):
        greet("heads", lax.rem(head + d, groups))
    expected = expected + groups - 1

    first_rows = pl.ds(0, rows)
    other_rows = pl.ds(rows, shard_len - rows)
    own_spot = pl.ds(own_keys, shard_len)
    loads = [
        pltpu.make_async_copy(k_hbm.at[0], keys.at[own_spot], load_sem.at[0]),
        pltpu.make_async_copy(q_hbm.at[0, first_rows], queries.at[first_rows], load_sem.at[1]),
        pltpu.make_async_copy(v_hbm.at[0], vals.at[own_spot], load_sem.at[2]),
        pltpu.make_async_copy(len_hbm, lens, load_sem.at[3]),
        pltpu.make_async_copy(q_hbm.at[0, other_rows], queries.at[other_rows], load_sem.at[4]),
    ]
    for load in loads:
        load.start()
    w_copy = pltpu.make_async_copy(w_hbm, w_ref, w_sem)
    w_copy.start()

    for d in range(1, reach + 1):
        @pl.when((me < d) & (me > 0))
        def _():
            spot = pl.ds((reach - d) * shard_len, shard_len)
            keys[spot, :] = jnp.zeros((shard_len, kv_width), keys.dtype)
            vals[spot, :] = jnp.zeros((shard_len, kv_width), vals.dtype)

    pl.semaphore_wait(barrier, expected)

    def kv_copies(d, target):
        spot = pl.ds((reach - d) * shard_len, shard_len)
        return [
            pltpu.make_async_remote_copy(
                src_ref=src.at[0], dst_ref=dst.at[spot],
                send_sem=kv_send.at[i, d - 1], recv_sem=kv_recv.at[i, d - 1],
                device_id={"seq": target}, device_id_type=MESH,
            )
            for i, (src, dst) in enumerate(((k_hbm, keys), (v_hbm, vals)))
        ]

    for d in range(1, reach + 1):
        @pl.when(me + d < seqs)
        def _():
            for copy in kv_copies(d, me + d):
                copy.start()

    for load in loads[:4]:
        load.wait()
    for d in range(1, reach + 1):
        @pl.when(me >= d)
        def _():
            for copy in kv_copies(d, me - d):
                copy.wait_recv()

    def slot_rows(source):
        return pl.ds(pl.multiple_of(source * rows, rows), rows)

    def z_copy(way, source, piece):
        target = b + 1 if way == 0 else b - 1
        here = piece + delay(jnp.abs(b - source))
        there = piece + delay(jnp.abs(target - source))
        return pltpu.make_async_remote_copy(
            src_ref=gath.at[here, slot_rows(source)],
            dst_ref=gath.at[there, slot_rows(source)],
            send_sem=z_send.at[way, source, piece], recv_sem=z_recv.at[source, piece],
            device_id={"batch": target}, device_id_type=MESH,
        )

    def z_arrival(source, piece):
        spot = gath.at[piece + delay(jnp.abs(b - source)), slot_rows(source)]
        return pltpu.make_async_copy(spot, spot, z_recv.at[source, piece])

    def goes(way, source):
        if way == 0:
            return (source <= b) & (b < n - 1)
        return (source >= b) & (b > 0)

    def pass_on(source, piece):
        for way in range(2):
            @pl.when(goes(way, source))
            def _():
                z_copy(way, source, piece).start()

    rate = HEAD_WIDTH ** (-0.5) * math.log2(math.e)
    shard_start = me * shard_len

    def attend(piece):
        base = pl.multiple_of(piece * rows, rows)
        row_pos = shard_start + base + lax.broadcasted_iota(jnp.int32, (rows, HEAD_WIDTH), 0)
        start = jnp.zeros((rows, HEAD_WIDTH), jnp.int32)
        end = jnp.int32(0)
        for d in range(DOCS):
            end = end + lens[0, d]
            start = jnp.where(row_pos >= end, end, start)

        def over(low):
            count = own_keys + shard_len - low
            key_pos = (
                shard_start - own_keys + low
                + lax.broadcasted_iota(jnp.int32, (rows, count), 1)
            )
            allowed = (key_pos >= start[:, :1]) & (key_pos <= row_pos[:, :1])
            bias = jnp.where(allowed, 0.0, -jnp.inf).astype(jnp.float32)
            bias = jnp.concatenate([bias] * per_kv, axis=0)
            for g in range(kv_heads):
                gcols = slice(g * HEAD_WIDTH, (g + 1) * HEAD_WIDTH)
                q = jnp.concatenate(
                    [
                        queries[pl.ds(base, rows), j * HEAD_WIDTH:(j + 1) * HEAD_WIDTH]
                        for j in range(g * per_kv, (g + 1) * per_kv)
                    ],
                    axis=0,
                )
                scores = lax.dot_general(
                    q, keys[low:, gcols], (((1,), (1,)), ((), ())),
                    preferred_element_type=jnp.float32,
                ) + bias
                weights = jnp.exp2((scores - jnp.max(scores, axis=1, keepdims=True)) * rate)
                total = jnp.sum(weights, axis=1, keepdims=True)
                summed = jnp.dot(
                    weights.astype(jnp.bfloat16), vals[low:, gcols],
                    preferred_element_type=jnp.float32,
                )
                result = (summed / total).astype(jnp.bfloat16)
                for i in range(per_kv):
                    j = g * per_kv + i
                    gath[piece, slot_rows(b), j * HEAD_WIDTH:(j + 1) * HEAD_WIDTH] = (
                        result[i * rows:(i + 1) * rows]
                    )

        if reach > 0:
            pl.when(me == 0)(functools.partial(over, own_keys))
            pl.when(me > 0)(functools.partial(over, 0))
        else:
            over(0)

    def part_copy(source, piece, slot, spot, cols):
        return pltpu.make_async_remote_copy(
            src_ref=stage.at[piece + delay(jnp.abs(b - source)), spot, cols],
            dst_ref=incoming.at[slot, piece, :, cols],
            send_sem=c_send.at[source, piece], recv_sem=c_recv.at[slot, piece],
            device_id={"heads": source}, device_id_type=MESH,
        )

    def part_to(source, piece, cols):
        slot = lax.rem(head - source - 1 + 2 * groups, groups)
        return part_copy(source, piece, slot, slot_rows(source), cols)

    all_cols = pl.ds(0, columns)
    last_delay = delay(jnp.maximum(b, n - 1 - b))

    def arrive(source, valid, piece):
        @pl.when(valid & (piece >= 0) & (piece < PIECES))
        def _():
            z_arrival(source, piece).wait()
            pass_on(source, piece)

    def project(r):
        for d in range(1, n):
            piece = r - max(d - 1, 0)
            arrive(b - d, b >= d, piece)
            arrive(b + d, b + d < n, piece)

        def tile(t, _):
            cols = pl.ds(pl.multiple_of(t * COLS, COLS), COLS)
            stage[r, :, cols] = jnp.dot(
                gath[r], w_ref[:, cols], preferred_element_type=jnp.float32
            ).astype(jnp.bfloat16)
            for source in range(n):
                piece = r - delay(jnp.abs(b - source))

                @pl.when((piece >= 0) & (piece < PIECES) & (head != source))
                def _():
                    part_to(source, piece, cols).start()

            return 0

        lax.fori_loop(0, blocks, tile, 0)

    def collect(piece, r):
        for slot in range(groups - 1):
            spot = incoming.at[slot, piece]
            pltpu.make_async_copy(spot, spot, c_recv.at[slot, piece]).wait()

        def tile(t, _):
            cols = pl.ds(pl.multiple_of(t * COLS, COLS), COLS)
            total = stage[r, slot_rows(head), cols].astype(jnp.float32)
            for slot in range(groups - 1):
                total = total + incoming[slot, piece, :, cols].astype(jnp.float32)
            out_ref[0, slot_rows(piece), cols] = total.astype(jnp.bfloat16)
            return 0

        lax.fori_loop(0, blocks, tile, 0)

    def step(i, _):
        @pl.when(i < PIECES)
        def _():
            @pl.when(i == 1)
            def _():
                loads[4].wait()

            attend(i)
            pass_on(b, i)

        @pl.when(i == AHEAD)
        def _():
            w_copy.wait()

        r = i - AHEAD

        @pl.when((r >= 0) & (r < PIECES + last_delay))
        def _():
            project(r)

        done = r - LAG
        piece = done - delay(jnp.abs(b - head))

        @pl.when((piece >= 0) & (piece < PIECES))
        def _():
            collect(piece, done)

        return 0

    lax.fori_loop(0, AHEAD + PIECES + max(n - 2, 0) + LAG, step, 0)

    for d in range(1, reach + 1):
        @pl.when(me + d < seqs)
        def _():
            for copy in kv_copies(d, me + d):
                copy.wait_send()

    def finish(piece, _):
        for source in range(n):
            for way in range(2):
                @pl.when(goes(way, source))
                def _():
                    z_copy(way, source, piece).wait_send()

            @pl.when(head != source)
            def _():
                part_to(source, piece, all_cols).wait_send()

        return 0

    lax.fori_loop(0, PIECES, finish, 0)


def solution(mesh):
    seqs, groups, n = mesh.shape["seq"], mesh.shape["heads"], mesh.shape["batch"]

    def per_device(queries, keys, values, doc_lengths, out_weight):
        shard_len, q_width = queries.shape[1:]
        kv_width = keys.shape[2]
        columns = out_weight.shape[1]
        seq_total = seqs * shard_len
        longest = seq_total // 2 + shard_len // 2
        reach = min((longest + shard_len - 2) // shard_len, seqs - 1)
        rows = shard_len // PIECES
        rounds = PIECES + max(n - 2, 0)
        key_count = (reach + 1) * shard_len
        hbm = pl.BlockSpec(memory_space=pltpu.HBM)
        dma = pltpu.SemaphoreType.DMA
        return pl.pallas_call(
            functools.partial(kernel, (seqs, groups, n, reach)),
            out_shape=jax.ShapeDtypeStruct((1, shard_len, columns), jnp.bfloat16),
            in_specs=[hbm] * 5,
            out_specs=pl.BlockSpec(memory_space=pltpu.VMEM),
            scratch_shapes=[
                pltpu.VMEM(out_weight.shape, jnp.bfloat16),
                pltpu.VMEM((shard_len, q_width), jnp.bfloat16),
                pltpu.VMEM((key_count, kv_width), jnp.bfloat16),
                pltpu.VMEM((key_count, kv_width), jnp.bfloat16),
                pltpu.SMEM(doc_lengths.shape, jnp.int32),
                pltpu.VMEM((rounds, n * rows, q_width), jnp.bfloat16),
                pltpu.VMEM((rounds, n * rows, columns), jnp.bfloat16),
                pltpu.VMEM((groups - 1, PIECES, rows, columns), jnp.bfloat16),
                dma,
                dma((5,)),
                dma((2, max(reach, 1))),
                dma((2, max(reach, 1))),
                dma((2, n, PIECES)),
                dma((n, PIECES)),
                dma((n, PIECES)),
                dma((groups - 1, PIECES)),
            ],
            compiler_params=pltpu.CompilerParams(
                collective_id=0, has_side_effects=True, vmem_limit_bytes=int(60 * 2**20)
            ),
        )(queries, keys, values, doc_lengths, out_weight)

    return jax.shard_map(
        per_device,
        mesh=mesh,
        in_specs=(
            P("batch", "seq", "heads"),
            P("batch", "seq", "heads"),
            P("batch", "seq", "heads"),
            P("batch", None),
            P("heads", "batch"),
        ),
        out_specs=P("heads", "seq", "batch"),
        check_vma=False,
    )
```

```python
import functools
import math

import jax
import jax.numpy as jnp
from jax import lax
from jax.experimental import pallas as pl
from jax.experimental.pallas import tpu as pltpu
from jax.sharding import PartitionSpec as P

HEAD_WIDTH = 128
DOCS = 16
PIECES = 16
HOP = 2
COLS = 1024
PARTS = 4
MESH = pl.DeviceIdType.MESH


def kernel(
    sizes, q_hbm, k_hbm, v_hbm, len_hbm, w_hbm, out_ref,
    w_ref, queries, keys, vals, lens, gath, stage, incoming, acc,
    w_sem, load_sem, kv_send, kv_recv, z_send, z_recv, c_send, c_recv,
):
    seqs, groups, n, reach = sizes
    shard_len, q_width = queries.shape
    kv_width = keys.shape[1]
    columns = w_ref.shape[1]
    kv_heads = kv_width // HEAD_WIDTH
    per_kv = q_width // kv_width
    rows = shard_len // PIECES
    pair = 2 * rows
    own_keys = reach * shard_len

    me = lax.axis_index("seq")
    head = lax.axis_index("heads")
    b = lax.axis_index("batch")

    barrier = pltpu.get_barrier_semaphore()

    def greet(axis, index):
        pl.semaphore_signal(barrier, inc=1, device_id={axis: index}, device_id_type=MESH)

    expected = 0
    for d in range(1, reach + 1):
        for cond, index in ((me >= d, me - d), (me + d < seqs, me + d)):
            expected = expected + cond.astype(jnp.int32)
            pl.when(cond)(functools.partial(greet, "seq", index))
    for cond, index in ((b > 0, b - 1), (b < n - 1, b + 1)):
        expected = expected + cond.astype(jnp.int32)
        pl.when(cond)(functools.partial(greet, "batch", index))
    for d in range(1, groups):
        greet("heads", lax.rem(head + d, groups))
    expected = expected + groups - 1

    first_rows = pl.ds(0, rows)
    other_rows = pl.ds(rows, shard_len - rows)
    own_spot = pl.ds(own_keys, shard_len)
    loads = [
        pltpu.make_async_copy(k_hbm.at[0], keys.at[own_spot], load_sem.at[0]),
        pltpu.make_async_copy(q_hbm.at[0, first_rows], queries.at[first_rows], load_sem.at[1]),
        pltpu.make_async_copy(v_hbm.at[0], vals.at[own_spot], load_sem.at[2]),
        pltpu.make_async_copy(len_hbm, lens, load_sem.at[3]),
        pltpu.make_async_copy(q_hbm.at[0, other_rows], queries.at[other_rows], load_sem.at[4]),
    ]
    for load in loads:
        load.start()
    w_copy = pltpu.make_async_copy(w_hbm, w_ref, w_sem)
    w_copy.start()

    for d in range(1, reach + 1):
        @pl.when((me < d) & (me > 0))
        def _():
            spot = pl.ds((reach - d) * shard_len, shard_len)
            keys[spot, :] = jnp.zeros((shard_len, kv_width), keys.dtype)
            vals[spot, :] = jnp.zeros((shard_len, kv_width), vals.dtype)

    pl.semaphore_wait(barrier, expected)

    def kv_copies(d, target):
        spot = pl.ds((reach - d) * shard_len, shard_len)
        return [
            pltpu.make_async_remote_copy(
                src_ref=src.at[0], dst_ref=dst.at[spot],
                send_sem=kv_send.at[i, d - 1], recv_sem=kv_recv.at[i, d - 1],
                device_id={"seq": target}, device_id_type=MESH,
            )
            for i, (src, dst) in enumerate(((k_hbm, keys), (v_hbm, vals)))
        ]

    for d in range(1, reach + 1):
        @pl.when(me + d < seqs)
        def _():
            for copy in kv_copies(d, me + d):
                copy.start()

    for load in loads[:4]:
        load.wait()
    for d in range(1, reach + 1):
        @pl.when(me >= d)
        def _():
            for copy in kv_copies(d, me - d):
                copy.wait_recv()

    deep = q_width // PARTS
    every = pl.ds(0, q_width)
    last = PIECES - 1

    def part_cols(part):
        return pl.ds(part * deep, deep)

    def pair_rows(index):
        return pl.ds(pl.multiple_of(index * pair, pair), pair)

    def piece_rows(piece):
        return pl.ds(pl.multiple_of(piece * rows, rows), rows)

    def place(source, piece):
        row = source * pair + lax.rem(piece, 2) * rows
        return lax.div(piece, 2), pl.ds(pl.multiple_of(row, rows), rows)

    def z_copy(way, source, piece, index, cols):
        spot = gath.at[*place(source, piece), cols]
        return pltpu.make_async_remote_copy(
            src_ref=spot, dst_ref=spot,
            send_sem=z_send.at[way, source], recv_sem=z_recv.at[source, index],
            device_id={"batch": b + 1 if way == 0 else b - 1}, device_id_type=MESH,
        )

    def z_wait(source, piece, index, cols):
        spot = gath.at[*place(source, piece), cols]
        pltpu.make_async_copy(spot, spot, z_recv.at[source, index]).wait()

    def goes(way, source):
        if way == 0:
            return (source <= b) & (b < n - 1)
        return (source >= b) & (b > 0)

    def move(way, source, piece, cond, own):
        cond = cond & goes(way, source) & (source >= 0) & (source < n)

        def go(index, cols):
            if not own:
                z_wait(source, piece, index, cols)
            z_copy(way, source, piece, index, cols).start()

        @pl.when(cond & (piece >= 0) & (piece < last))
        def _():
            go(piece, every)

        late = b == (n - 2 if way == 0 else 1)

        @pl.when(cond & (piece == last) & jnp.logical_not(late))
        def _():
            for part in range(PARTS):
                go(last + part, part_cols(part))

    rate = HEAD_WIDTH ** (-0.5) * math.log2(math.e)
    shard_start = me * shard_len

    def attend(piece):
        base = pl.multiple_of(piece * rows, rows)
        row_pos = shard_start + base + lax.broadcasted_iota(jnp.int32, (rows, HEAD_WIDTH), 0)
        start = jnp.zeros((rows, HEAD_WIDTH), jnp.int32)
        end = jnp.int32(0)
        for d in range(DOCS):
            end = end + lens[0, d]
            start = jnp.where(row_pos >= end, end, start)

        def over(low):
            count = own_keys + shard_len - low
            key_pos = (
                shard_start - own_keys + low
                + lax.broadcasted_iota(jnp.int32, (rows, count), 1)
            )
            allowed = (key_pos >= start[:, :1]) & (key_pos <= row_pos[:, :1])
            bias = jnp.where(allowed, 0.0, -jnp.inf).astype(jnp.float32)
            bias = jnp.concatenate([bias] * per_kv, axis=0)
            for g in range(kv_heads):
                gcols = slice(g * HEAD_WIDTH, (g + 1) * HEAD_WIDTH)
                q = jnp.concatenate(
                    [
                        queries[pl.ds(base, rows), j * HEAD_WIDTH:(j + 1) * HEAD_WIDTH]
                        for j in range(g * per_kv, (g + 1) * per_kv)
                    ],
                    axis=0,
                )
                scores = lax.dot_general(
                    q, keys[low:, gcols], (((1,), (1,)), ((), ())),
                    preferred_element_type=jnp.float32,
                ) + bias
                weights = jnp.exp2((scores - jnp.max(scores, axis=1, keepdims=True)) * rate)
                total = jnp.sum(weights, axis=1, keepdims=True)
                summed = jnp.dot(
                    weights.astype(jnp.bfloat16), vals[low:, gcols],
                    preferred_element_type=jnp.float32,
                )
                result = (summed / total).astype(jnp.bfloat16)
                for i in range(per_kv):
                    j = g * per_kv + i
                    gath[*place(b, piece), j * HEAD_WIDTH:(j + 1) * HEAD_WIDTH] = (
                        result[i * rows:(i + 1) * rows]
                    )

        if reach > 0:
            pl.when(me == 0)(functools.partial(over, own_keys))
            pl.when(me > 0)(functools.partial(over, 0))
        else:
            over(0)

    at_end = (b == 0) | (b == n - 1)

    def part_send(source, index, here, there, sem, cols):
        slot = lax.rem(head - source - 1 + 2 * groups, groups)

        @pl.when(head != source)
        def _():
            pltpu.make_async_remote_copy(
                src_ref=stage.at[index, here, cols],
                dst_ref=incoming.at[slot, there, cols],
                send_sem=c_send.at[source], recv_sem=c_recv.at[slot, sem],
                device_id={"heads": source}, device_id_type=MESH,
            ).start()

    def over_tiles(body, width=COLS):
        def tile(t, _):
            body(pl.ds(pl.multiple_of(t * width, width), width))
            return 0

        lax.fori_loop(0, columns // width, tile, 0)

    def product(lhs, depth, cols):
        return jnp.dot(lhs, w_ref[depth, cols], preferred_element_type=jnp.float32)

    def project_pair(index):
        for source in range(n):
            @pl.when(at_end & (source != b))
            def _():
                z_wait(source, 2 * index, 2 * index, every)
                z_wait(source, 2 * index + 1, 2 * index + 1, every)

        def body(cols):
            stage[index, :, cols] = product(gath[index], every, cols).astype(jnp.bfloat16)
            for source in range(n):
                spot = pl.ds(source * pair, pair)
                part_send(source, index, spot, pair_rows(index), index, cols)

        over_tiles(body)

    half = PIECES // 2 - 1

    def spots(piece):
        return [pl.ds(s * pair + (piece % 2) * rows, rows) for s in range(n)]

    def project_one():
        piece = last - 1
        for source in range(n):
            @pl.when(at_end & (source != b))
            def _():
                z_wait(source, piece, piece, every)

        def body(cols):
            lhs = jnp.concatenate([gath[half, spot, :] for spot in spots(piece)], axis=0)
            part = product(lhs, every, cols).astype(jnp.bfloat16)
            for source, spot in enumerate(spots(piece)):
                stage[half, spot, cols] = part[source * rows:(source + 1) * rows]
                part_send(source, half, spot, pl.ds(piece * rows, rows), half, cols)

        over_tiles(body)

    def project_last():
        for part in range(PARTS):
            for source in range(n):
                @pl.when(at_end & (source != b))
                def _():
                    z_wait(source, last, last + part, part_cols(part))

            def body(cols):
                lhs = jnp.concatenate(
                    [gath[half, spot, part_cols(part)] for spot in spots(last)], axis=0
                )
                total = product(lhs, part_cols(part), cols)
                if part > 0:
                    total = total + acc[:, cols]
                if part < PARTS - 1:
                    acc[:, cols] = total
                    return
                total = total.astype(jnp.bfloat16)
                for source, spot in enumerate(spots(last)):
                    stage[half, spot, cols] = total[source * rows:(source + 1) * rows]
                    part_send(source, half, spot, pl.ds(last * rows, rows), half + 1, cols)

            over_tiles(body, COLS if part == PARTS - 1 else 2 * COLS)

    def collect(index, here, there, sem):
        for slot in range(groups - 1):
            spot = incoming.at[slot, there]
            pltpu.make_async_copy(spot, spot, c_recv.at[slot, sem]).wait()

        def body(cols):
            total = stage[index, here, cols].astype(jnp.float32)
            for slot in range(groups - 1):
                total = total + incoming[slot, there, cols].astype(jnp.float32)
            out_ref[0, there, cols] = total.astype(jnp.bfloat16)

        over_tiles(body)

    def collect_one(piece, sem):
        collect(*place(head, piece), piece_rows(piece), sem)

    behind = (n - 1) * HOP
    hold = (n - 2) * HOP

    def step(i, _):
        @pl.when(i < PIECES)
        def _():
            @pl.when(i == 1)
            def _():
                loads[4].wait()

            attend(i)

        for way in range(2):
            late = b == (n - 2 if way == 0 else 1)
            for d in range(n - 1):
                source = b - d if way == 0 else b + d
                begin = hold + sum(hold - e * HOP for e in range(d))
                early = i - d * HOP
                kept = i - hold
                move(
                    way, source, early,
                    jnp.logical_not(late) | (i < begin) | (d == n - 2), d == 0,
                )
                if d < n - 2:
                    move(
                        way, source, kept,
                        late & (kept >= begin - d * HOP) & (kept < last), d == 0,
                    )

            @pl.when(late & (i == last + hold))
            def _():
                for part in range(PARTS):
                    for d in range(n - 1):
                        source = b - d if way == 0 else b + d
                        if d > 0:
                            z_wait(source, last, last + part, part_cols(part))
                        z_copy(way, source, last, last + part, part_cols(part)).start()

        @pl.when(i == behind)
        def _():
            w_copy.wait()

        r = i - behind
        odd = lax.rem(jnp.maximum(r, 0), 2) == 1
        index = lax.div(jnp.maximum(r, 0), 2)

        @pl.when(odd & (r < last))
        def _():
            project_pair(index)

        @pl.when(r == last - 1)
        def _():
            project_one()

        @pl.when(r == last)
        def _():
            project_last()

        @pl.when(odd & (r >= 3) & (r <= last))
        def _():
            collect(index - 1, pair_rows(head), pair_rows(index - 1), index - 1)

        return 0

    lax.fori_loop(0, behind + PIECES, step, 0)
    collect_one(last - 1, half)
    collect_one(last, half + 1)

    for d in range(1, reach + 1):
        @pl.when(me + d < seqs)
        def _():
            for copy in kv_copies(d, me + d):
                copy.wait_send()

    def drain(like, sem):
        pltpu.make_async_copy(like, like, sem).wait()

    for source in range(n):
        for way in range(2):
            @pl.when(goes(way, source))
            def _():
                drain(queries, z_send.at[way, source])

        @pl.when(head != source)
        def _():
            drain(out_ref.at[0], c_send.at[source])


def solution(mesh):
    seqs, groups, n = mesh.shape["seq"], mesh.shape["heads"], mesh.shape["batch"]

    def per_device(queries, keys, values, doc_lengths, out_weight):
        shard_len, q_width = queries.shape[1:]
        kv_width = keys.shape[2]
        columns = out_weight.shape[1]
        seq_total = seqs * shard_len
        longest = seq_total // 2 + shard_len // 2
        reach = min((longest + shard_len - 2) // shard_len, seqs - 1)
        rows = shard_len // PIECES
        pairs = PIECES // 2
        key_count = (reach + 1) * shard_len
        hbm = pl.BlockSpec(memory_space=pltpu.HBM)
        dma = pltpu.SemaphoreType.DMA
        return pl.pallas_call(
            functools.partial(kernel, (seqs, groups, n, reach)),
            out_shape=pltpu.VMEM((1, shard_len, columns), jnp.bfloat16),
            in_specs=[hbm] * 5,
            out_specs=pl.BlockSpec(memory_space=pltpu.VMEM),
            scratch_shapes=[
                pltpu.VMEM(out_weight.shape, jnp.bfloat16),
                pltpu.VMEM((shard_len, q_width), jnp.bfloat16),
                pltpu.VMEM((key_count, kv_width), jnp.bfloat16),
                pltpu.VMEM((key_count, kv_width), jnp.bfloat16),
                pltpu.SMEM(doc_lengths.shape, jnp.int32),
                pltpu.VMEM((pairs, 2 * n * rows, q_width), jnp.bfloat16),
                pltpu.VMEM((pairs, 2 * n * rows, columns), jnp.bfloat16),
                pltpu.VMEM((groups - 1, shard_len, columns), jnp.bfloat16),
                pltpu.VMEM((n * rows, columns), jnp.float32),
                dma,
                dma((5,)),
                dma((2, max(reach, 1))),
                dma((2, max(reach, 1))),
                dma((2, n)),
                dma((n, PIECES - 1 + PARTS)),
                dma((n,)),
                dma((groups - 1, pairs + 1)),
            ],
            compiler_params=pltpu.CompilerParams(
                collective_id=0, has_side_effects=True, vmem_limit_bytes=48 * 2**20
            ),
        )(*(
            pltpu.with_memory_space_constraint(x, pltpu.HBM)
            for x in (queries, keys, values, doc_lengths, out_weight)
        ))

    return jax.shard_map(
        per_device,
        mesh=mesh,
        in_specs=(
            P("batch", "seq", "heads"),
            P("batch", "seq", "heads"),
            P("batch", "seq", "heads"),
            P("batch", None),
            P("heads", "batch"),
        ),
        out_specs=P("heads", "seq", "batch"),
        check_vma=False,
    )
```

```python
import functools
import math

import jax
import jax.numpy as jnp
from jax import lax
from jax.experimental import pallas as pl
from jax.experimental.pallas import tpu as pltpu
from jax.sharding import PartitionSpec as P

HEAD_WIDTH = 128
DOCS = 16
PIECES = 16
HOP = 2
COLS = 1024
PARTS = 4
MESH = pl.DeviceIdType.MESH


def kernel(
    sizes, q_hbm, k_hbm, v_hbm, len_hbm, w_hbm, out_ref,
    w_ref, queries, keys, vals, lens, gath, stage, incoming, acc,
    w_sem, load_sem, kv_send, kv_recv, z_send, z_recv, c_send, c_recv,
):
    seqs, groups, n, reach = sizes
    shard_len, q_width = queries.shape
    kv_width = keys.shape[1]
    columns = w_ref.shape[1]
    kv_heads = kv_width // HEAD_WIDTH
    per_kv = q_width // kv_width
    rows = shard_len // PIECES
    pair = 2 * rows
    own_keys = reach * shard_len

    me = lax.axis_index("seq")
    head = lax.axis_index("heads")
    b = lax.axis_index("batch")

    barrier = pltpu.get_barrier_semaphore()

    def greet(axis, index):
        pl.semaphore_signal(barrier, inc=1, device_id={axis: index}, device_id_type=MESH)

    for d in range(groups - 1, 0, -1):
        greet("heads", lax.rem(head + d, groups))
    expected = groups - 1
    for cond, index in ((b > 0, b - 1), (b < n - 1, b + 1)):
        expected = expected + cond.astype(jnp.int32)
        pl.when(cond)(functools.partial(greet, "batch", index))
    for d in range(1, reach + 1):
        for cond, index in ((me >= d, me - d), (me + d < seqs, me + d)):
            expected = expected + cond.astype(jnp.int32)
            pl.when(cond)(functools.partial(greet, "seq", index))

    first_rows = pl.ds(0, rows)
    other_rows = pl.ds(rows, shard_len - rows)
    own_spot = pl.ds(own_keys, shard_len)
    loads = [
        pltpu.make_async_copy(k_hbm.at[0], keys.at[own_spot], load_sem.at[0]),
        pltpu.make_async_copy(q_hbm.at[0, first_rows], queries.at[first_rows], load_sem.at[1]),
        pltpu.make_async_copy(v_hbm.at[0], vals.at[own_spot], load_sem.at[2]),
        pltpu.make_async_copy(len_hbm, lens, load_sem.at[3]),
        pltpu.make_async_copy(q_hbm.at[0, other_rows], queries.at[other_rows], load_sem.at[4]),
    ]
    for load in loads:
        load.start()
    w_copy = pltpu.make_async_copy(w_hbm, w_ref, w_sem)
    w_copy.start()

    for d in range(1, reach + 1):
        @pl.when((me < d) & (me > 0))
        def _():
            spot = pl.ds((reach - d) * shard_len, shard_len)
            keys[spot, :] = jnp.zeros((shard_len, kv_width), keys.dtype)
            vals[spot, :] = jnp.zeros((shard_len, kv_width), vals.dtype)

    deep = q_width // PARTS
    every = pl.ds(0, q_width)
    last = PIECES - 1

    def part_cols(part):
        return pl.ds(part * deep, deep)

    def pair_rows(index):
        return pl.ds(pl.multiple_of(index * pair, pair), pair)

    def piece_rows(piece):
        return pl.ds(pl.multiple_of(piece * rows, rows), rows)

    def place(source, piece):
        row = source * pair + lax.rem(piece, 2) * rows
        return lax.div(piece, 2), pl.ds(pl.multiple_of(row, rows), rows)

    def z_copy(way, source, piece, index, cols):
        spot = gath.at[*place(source, piece), cols]
        return pltpu.make_async_remote_copy(
            src_ref=spot, dst_ref=spot,
            send_sem=z_send.at[way, source], recv_sem=z_recv.at[source, index],
            device_id={"batch": b + 1 if way == 0 else b - 1}, device_id_type=MESH,
        )

    def z_wait(source, piece, index, cols):
        spot = gath.at[*place(source, piece), cols]
        pltpu.make_async_copy(spot, spot, z_recv.at[source, index]).wait()

    def goes(way, source):
        if way == 0:
            return (source <= b) & (b < n - 1)
        return (source >= b) & (b > 0)

    def move(way, source, piece, cond, own):
        cond = cond & goes(way, source) & (source >= 0) & (source < n)

        def go(index, cols):
            if not own:
                z_wait(source, piece, index, cols)
            z_copy(way, source, piece, index, cols).start()

        @pl.when(cond & (piece >= 0) & (piece < last))
        def _():
            go(piece, every)

        late = b == (n - 2 if way == 0 else 1)

        @pl.when(cond & (piece == last) & jnp.logical_not(late))
        def _():
            for part in range(PARTS):
                go(last + part, part_cols(part))

    rate = HEAD_WIDTH ** (-0.5) * math.log2(math.e)
    shard_start = me * shard_len

    def attend(piece):
        base = pl.multiple_of(piece * rows, rows)
        row_pos = shard_start + base + lax.broadcasted_iota(jnp.int32, (rows, HEAD_WIDTH), 0)
        start = jnp.zeros((rows, HEAD_WIDTH), jnp.int32)
        end = jnp.int32(0)
        for d in range(DOCS):
            end = end + lens[0, d]
            start = jnp.where(row_pos >= end, end, start)

        def over(low, high):
            count = high - low
            key_pos = (
                shard_start - own_keys + low
                + lax.broadcasted_iota(jnp.int32, (rows, count), 1)
            )
            allowed = (key_pos >= start[:, :1]) & (key_pos <= row_pos[:, :1])
            bias = jnp.where(allowed, 0.0, -jnp.inf).astype(jnp.float32)
            bias = jnp.concatenate([bias] * per_kv, axis=0)
            for g in range(kv_heads):
                gcols = slice(g * HEAD_WIDTH, (g + 1) * HEAD_WIDTH)
                q = jnp.concatenate(
                    [
                        queries[pl.ds(base, rows), j * HEAD_WIDTH:(j + 1) * HEAD_WIDTH]
                        for j in range(g * per_kv, (g + 1) * per_kv)
                    ],
                    axis=0,
                )
                scores = lax.dot_general(
                    q, keys[low:high, gcols], (((1,), (1,)), ((), ())),
                    preferred_element_type=jnp.float32,
                ) + bias
                weights = jnp.exp2((scores - jnp.max(scores, axis=1, keepdims=True)) * rate)
                total = jnp.sum(weights, axis=1, keepdims=True)
                summed = jnp.dot(
                    weights.astype(jnp.bfloat16), vals[low:high, gcols],
                    preferred_element_type=jnp.float32,
                )
                result = (summed / total).astype(jnp.bfloat16)
                for i in range(per_kv):
                    j = g * per_kv + i
                    gath[*place(b, piece), j * HEAD_WIDTH:(j + 1) * HEAD_WIDTH] = (
                        result[i * rows:(i + 1) * rows]
                    )

        middle, top = own_keys + shard_len // 2, own_keys + shard_len
        if isinstance(piece, int):
            over(own_keys, middle)
            return
        soon = piece < PIECES // 2
        for cond, high in ((soon, middle), (jnp.logical_not(soon), top)):
            pl.when(cond & (me == 0))(functools.partial(over, own_keys, high))
            if reach > 0:
                pl.when(cond & (me > 0))(functools.partial(over, 0, high))

    for load in loads[:4]:
        load.wait()

    @pl.when(me == 0)
    def _():
        attend(0)

    pl.semaphore_wait(barrier, expected)

    def kv_copies(d, target):
        spot = pl.ds((reach - d) * shard_len, shard_len)
        return [
            pltpu.make_async_remote_copy(
                src_ref=src.at[0], dst_ref=dst.at[spot],
                send_sem=kv_send.at[i, d - 1], recv_sem=kv_recv.at[i, d - 1],
                device_id={"seq": target}, device_id_type=MESH,
            )
            for i, (src, dst) in enumerate(((k_hbm, keys), (v_hbm, vals)))
        ]

    for d in range(1, reach + 1):
        @pl.when(me + d < seqs)
        def _():
            for copy in kv_copies(d, me + d):
                copy.start()

    for d in range(1, reach + 1):
        @pl.when(me >= d)
        def _():
            for copy in kv_copies(d, me - d):
                copy.wait_recv()

    at_end = (b == 0) | (b == n - 1)

    def part_send(source, index, here, there, sem, cols):
        slot = lax.rem(head - source - 1 + 2 * groups, groups)

        @pl.when(head != source)
        def _():
            pltpu.make_async_remote_copy(
                src_ref=stage.at[index, here, cols],
                dst_ref=incoming.at[slot, there, cols],
                send_sem=c_send.at[source], recv_sem=c_recv.at[slot, sem],
                device_id={"heads": source}, device_id_type=MESH,
            ).start()

    def over_tiles(body, width=COLS):
        def tile(t, _):
            body(pl.ds(pl.multiple_of(t * width, width), width))
            return 0

        lax.fori_loop(0, columns // width, tile, 0)

    def product(lhs, depth, cols):
        return jnp.dot(lhs, w_ref[depth, cols], preferred_element_type=jnp.float32)

    def project_pair(index):
        for source in range(n):
            @pl.when(at_end & (source != b))
            def _():
                z_wait(source, 2 * index, 2 * index, every)
                z_wait(source, 2 * index + 1, 2 * index + 1, every)

        def body(cols):
            stage[index, :, cols] = product(gath[index], every, cols).astype(jnp.bfloat16)
            for source in range(n):
                spot = pl.ds(source * pair, pair)
                part_send(source, index, spot, pair_rows(index), index, cols)

        over_tiles(body)

    half = PIECES // 2 - 1

    def spots(piece):
        return [pl.ds(s * pair + (piece % 2) * rows, rows) for s in range(n)]

    def project_one():
        piece = last - 1
        for source in range(n):
            @pl.when(at_end & (source != b))
            def _():
                z_wait(source, piece, piece, every)

        def body(cols):
            lhs = jnp.concatenate([gath[half, spot, :] for spot in spots(piece)], axis=0)
            part = product(lhs, every, cols).astype(jnp.bfloat16)
            for source, spot in enumerate(spots(piece)):
                stage[half, spot, cols] = part[source * rows:(source + 1) * rows]
                part_send(source, half, spot, pl.ds(piece * rows, rows), half, cols)

        over_tiles(body)

    def project_last():
        for part in range(PARTS):
            for source in range(n):
                @pl.when(at_end & (source != b))
                def _():
                    z_wait(source, last, last + part, part_cols(part))

            def body(cols):
                lhs = jnp.concatenate(
                    [gath[half, spot, part_cols(part)] for spot in spots(last)], axis=0
                )
                total = product(lhs, part_cols(part), cols)
                if part > 0:
                    total = total + acc[:, cols]
                if part < PARTS - 1:
                    acc[:, cols] = total
                    return
                total = total.astype(jnp.bfloat16)
                for source, spot in enumerate(spots(last)):
                    stage[half, spot, cols] = total[source * rows:(source + 1) * rows]
                    part_send(source, half, spot, pl.ds(last * rows, rows), half + 1, cols)

            over_tiles(body, COLS if part == PARTS - 1 else 2 * COLS)

    def collect(index, here, there, sem):
        for slot in range(groups - 1):
            spot = incoming.at[slot, there]
            pltpu.make_async_copy(spot, spot, c_recv.at[slot, sem]).wait()

        def body(cols):
            total = stage[index, here, cols].astype(jnp.float32)
            for slot in range(groups - 1):
                total = total + incoming[slot, there, cols].astype(jnp.float32)
            out_ref[0, there, cols] = total.astype(jnp.bfloat16)

        over_tiles(body)

    def collect_one(piece, sem):
        collect(*place(head, piece), piece_rows(piece), sem)

    behind = (n - 1) * HOP
    hold = (n - 2) * HOP

    def step(i, _):
        @pl.when(i < PIECES)
        def _():
            @pl.when(i == 1)
            def _():
                loads[4].wait()

            @pl.when((i > 0) | (me > 0))
            def _():
                attend(i)

        for way in range(2):
            late = b == (n - 2 if way == 0 else 1)
            for d in range(n - 1):
                source = b - d if way == 0 else b + d
                begin = hold + sum(hold - e * HOP for e in range(d))
                early = i - d * HOP
                kept = i - hold
                move(
                    way, source, early,
                    jnp.logical_not(late) | (i < begin) | (d == n - 2), d == 0,
                )
                if d < n - 2:
                    move(
                        way, source, kept,
                        late & (kept >= begin - d * HOP) & (kept < last), d == 0,
                    )

            @pl.when(late & (i == last + hold))
            def _():
                for part in range(PARTS):
                    for d in range(n - 1):
                        source = b - d if way == 0 else b + d
                        if d > 0:
                            z_wait(source, last, last + part, part_cols(part))
                        z_copy(way, source, last, last + part, part_cols(part)).start()

        @pl.when(i == behind)
        def _():
            w_copy.wait()

        r = i - behind
        odd = lax.rem(jnp.maximum(r, 0), 2) == 1
        index = lax.div(jnp.maximum(r, 0), 2)

        @pl.when(odd & (r < last))
        def _():
            project_pair(index)

        @pl.when(r == last - 1)
        def _():
            project_one()

        @pl.when(r == last)
        def _():
            project_last()

        @pl.when(odd & (r >= 3) & (r <= last))
        def _():
            collect(index - 1, pair_rows(head), pair_rows(index - 1), index - 1)

        return 0

    lax.fori_loop(0, behind + PIECES, step, 0)
    collect_one(last - 1, half)
    collect_one(last, half + 1)

    for d in range(1, reach + 1):
        @pl.when(me + d < seqs)
        def _():
            for copy in kv_copies(d, me + d):
                copy.wait_send()

    def drain(like, sem):
        pltpu.make_async_copy(like, like, sem).wait()

    for source in range(n):
        for way in range(2):
            @pl.when(goes(way, source))
            def _():
                drain(queries, z_send.at[way, source])

        @pl.when(head != source)
        def _():
            drain(out_ref.at[0], c_send.at[source])


def solution(mesh):
    seqs, groups, n = mesh.shape["seq"], mesh.shape["heads"], mesh.shape["batch"]

    def per_device(queries, keys, values, doc_lengths, out_weight):
        shard_len, q_width = queries.shape[1:]
        kv_width = keys.shape[2]
        columns = out_weight.shape[1]
        seq_total = seqs * shard_len
        longest = seq_total // 2 + shard_len // 2
        reach = min((longest + shard_len - 2) // shard_len, seqs - 1)
        rows = shard_len // PIECES
        pairs = PIECES // 2
        key_count = (reach + 1) * shard_len
        hbm = pl.BlockSpec(memory_space=pltpu.HBM)
        dma = pltpu.SemaphoreType.DMA
        return pl.pallas_call(
            functools.partial(kernel, (seqs, groups, n, reach)),
            out_shape=pltpu.VMEM((1, shard_len, columns), jnp.bfloat16),
            in_specs=[hbm] * 5,
            out_specs=pl.BlockSpec(memory_space=pltpu.VMEM),
            scratch_shapes=[
                pltpu.VMEM(out_weight.shape, jnp.bfloat16),
                pltpu.VMEM((shard_len, q_width), jnp.bfloat16),
                pltpu.VMEM((key_count, kv_width), jnp.bfloat16),
                pltpu.VMEM((key_count, kv_width), jnp.bfloat16),
                pltpu.SMEM(doc_lengths.shape, jnp.int32),
                pltpu.VMEM((pairs, 2 * n * rows, q_width), jnp.bfloat16),
                pltpu.VMEM((pairs, 2 * n * rows, columns), jnp.bfloat16),
                pltpu.VMEM((groups - 1, shard_len, columns), jnp.bfloat16),
                pltpu.VMEM((n * rows, columns), jnp.float32),
                dma,
                dma((5,)),
                dma((2, max(reach, 1))),
                dma((2, max(reach, 1))),
                dma((2, n)),
                dma((n, PIECES - 1 + PARTS)),
                dma((n,)),
                dma((groups - 1, pairs + 1)),
            ],
            compiler_params=pltpu.CompilerParams(
                collective_id=0, has_side_effects=True, vmem_limit_bytes=48 * 2**20
            ),
        )(*(
            pltpu.with_memory_space_constraint(x, pltpu.HBM)
            for x in (queries, keys, values, doc_lengths, out_weight)
        ))

    return jax.shard_map(
        per_device,
        mesh=mesh,
        in_specs=(
            P("batch", "seq", "heads"),
            P("batch", "seq", "heads"),
            P("batch", "seq", "heads"),
            P("batch", None),
            P("heads", "batch"),
        ),
        out_specs=P("heads", "seq", "batch"),
        check_vma=False,
    )
```

```python
import functools
import math

import jax
import jax.numpy as jnp
from jax import lax
from jax.experimental import pallas as pl
from jax.experimental.pallas import tpu as pltpu
from jax.sharding import PartitionSpec as P

HEAD_WIDTH = 128
DOCS = 16
PIECES = 16
HOP = 2
COLS = 1024
PARTS = 4
MESH = pl.DeviceIdType.MESH


def kernel(
    sizes, q_hbm, k_hbm, v_hbm, len_hbm, w_hbm, out_ref,
    w_ref, queries, keys, vals, lens, gath, stage, incoming, acc,
    w_sem, load_sem, kv_send, kv_recv, z_send, z_recv, c_send, c_recv,
):
    seqs, groups, n, reach = sizes
    shard_len, q_width = queries.shape
    kv_width = keys.shape[1]
    columns = w_ref.shape[1]
    kv_heads = kv_width // HEAD_WIDTH
    per_kv = q_width // kv_width
    rows = shard_len // PIECES
    pair = 2 * rows
    own_keys = reach * shard_len

    me = lax.axis_index("seq")
    head = lax.axis_index("heads")
    b = lax.axis_index("batch")

    barrier = pltpu.get_barrier_semaphore()

    def greet(axis, index):
        pl.semaphore_signal(barrier, inc=1, device_id={axis: index}, device_id_type=MESH)

    for d in range(groups - 1, 0, -1):
        greet("heads", lax.rem(head + d, groups))
    expected = groups - 1
    for cond, index in ((b > 0, b - 1), (b < n - 1, b + 1)):
        expected = expected + cond.astype(jnp.int32)
        pl.when(cond)(functools.partial(greet, "batch", index))
    for d in range(1, reach + 1):
        for cond, index in ((me >= d, me - d), (me + d < seqs, me + d)):
            expected = expected + cond.astype(jnp.int32)
            pl.when(cond)(functools.partial(greet, "seq", index))

    first_rows = pl.ds(0, rows)
    other_rows = pl.ds(rows, shard_len - rows)
    own_spot = pl.ds(own_keys, shard_len)
    loads = [
        pltpu.make_async_copy(k_hbm.at[0], keys.at[own_spot], load_sem.at[0]),
        pltpu.make_async_copy(q_hbm.at[0, first_rows], queries.at[first_rows], load_sem.at[1]),
        pltpu.make_async_copy(v_hbm.at[0], vals.at[own_spot], load_sem.at[2]),
        pltpu.make_async_copy(len_hbm, lens, load_sem.at[3]),
        pltpu.make_async_copy(q_hbm.at[0, other_rows], queries.at[other_rows], load_sem.at[4]),
    ]
    for load in loads:
        load.start()
    w_copy = pltpu.make_async_copy(w_hbm, w_ref, w_sem)

    for d in range(1, reach + 1):
        @pl.when((me < d) & (me > 0))
        def _():
            spot = pl.ds((reach - d) * shard_len, shard_len)
            keys[spot, :] = jnp.zeros((shard_len, kv_width), keys.dtype)
            vals[spot, :] = jnp.zeros((shard_len, kv_width), vals.dtype)

    deep = q_width // PARTS
    every = pl.ds(0, q_width)
    last = PIECES - 1

    def part_cols(part):
        return pl.ds(part * deep, deep)

    def pair_rows(index):
        return pl.ds(pl.multiple_of(index * pair, pair), pair)

    def piece_rows(piece):
        return pl.ds(pl.multiple_of(piece * rows, rows), rows)

    def place(source, piece):
        row = source * pair + lax.rem(piece, 2) * rows
        return lax.div(piece, 2), pl.ds(pl.multiple_of(row, rows), rows)

    def z_copy(way, source, piece, index, cols):
        spot = gath.at[*place(source, piece), cols]
        return pltpu.make_async_remote_copy(
            src_ref=spot, dst_ref=spot,
            send_sem=z_send.at[way, source], recv_sem=z_recv.at[source, index],
            device_id={"batch": b + 1 if way == 0 else b - 1}, device_id_type=MESH,
        )

    def z_wait(source, piece, index, cols):
        spot = gath.at[*place(source, piece), cols]
        pltpu.make_async_copy(spot, spot, z_recv.at[source, index]).wait()

    def goes(way, source):
        if way == 0:
            return (source <= b) & (b < n - 1)
        return (source >= b) & (b > 0)

    def move(way, source, piece, cond, own):
        cond = cond & goes(way, source) & (source >= 0) & (source < n)

        def go(index, cols):
            if not own:
                z_wait(source, piece, index, cols)
            z_copy(way, source, piece, index, cols).start()

        @pl.when(cond & (piece >= 0) & (piece < last))
        def _():
            go(piece, every)

        late = b == (n - 2 if way == 0 else 1)

        @pl.when(cond & (piece == last) & jnp.logical_not(late))
        def _():
            for part in range(PARTS):
                go(last + part, part_cols(part))

    rate = HEAD_WIDTH ** (-0.5) * math.log2(math.e)
    shard_start = me * shard_len

    def attend(piece):
        base = pl.multiple_of(piece * rows, rows)
        row_pos = shard_start + base + lax.broadcasted_iota(jnp.int32, (rows, HEAD_WIDTH), 0)
        start = jnp.zeros((rows, HEAD_WIDTH), jnp.int32)
        end = jnp.int32(0)
        for d in range(DOCS):
            end = end + lens[0, d]
            start = jnp.where(row_pos >= end, end, start)

        def over(low, high):
            count = high - low
            key_pos = (
                shard_start - own_keys + low
                + lax.broadcasted_iota(jnp.int32, (rows, count), 1)
            )
            allowed = (key_pos >= start[:, :1]) & (key_pos <= row_pos[:, :1])
            bias = jnp.where(allowed, 0.0, -jnp.inf).astype(jnp.float32)
            bias = jnp.concatenate([bias] * per_kv, axis=0)
            for g in range(kv_heads):
                gcols = slice(g * HEAD_WIDTH, (g + 1) * HEAD_WIDTH)
                q = jnp.concatenate(
                    [
                        queries[pl.ds(base, rows), j * HEAD_WIDTH:(j + 1) * HEAD_WIDTH]
                        for j in range(g * per_kv, (g + 1) * per_kv)
                    ],
                    axis=0,
                )
                scores = lax.dot_general(
                    q, keys[low:high, gcols], (((1,), (1,)), ((), ())),
                    preferred_element_type=jnp.float32,
                ) + bias
                weights = jnp.exp2((scores - jnp.max(scores, axis=1, keepdims=True)) * rate)
                total = jnp.sum(weights, axis=1, keepdims=True)
                summed = jnp.dot(
                    weights.astype(jnp.bfloat16), vals[low:high, gcols],
                    preferred_element_type=jnp.float32,
                )
                result = (summed / total).astype(jnp.bfloat16)
                for i in range(per_kv):
                    j = g * per_kv + i
                    gath[*place(b, piece), j * HEAD_WIDTH:(j + 1) * HEAD_WIDTH] = (
                        result[i * rows:(i + 1) * rows]
                    )

        middle, top = own_keys + shard_len // 2, own_keys + shard_len
        if isinstance(piece, int):
            over(own_keys, middle)
            return
        soon = piece < PIECES // 2
        for cond, high in ((soon, middle), (jnp.logical_not(soon), top)):
            pl.when(cond & (me == 0))(functools.partial(over, own_keys, high))
            if reach > 0:
                pl.when(cond & (me > 0))(functools.partial(over, 0, high))

    for load in loads[:4]:
        load.wait()

    @pl.when(me == 0)
    def _():
        attend(0)

    pl.semaphore_wait(barrier, expected)

    def kv_copies(d, target):
        spot = pl.ds((reach - d) * shard_len, shard_len)
        return [
            pltpu.make_async_remote_copy(
                src_ref=src.at[0], dst_ref=dst.at[spot],
                send_sem=kv_send.at[i, d - 1], recv_sem=kv_recv.at[i, d - 1],
                device_id={"seq": target}, device_id_type=MESH,
            )
            for i, (src, dst) in enumerate(((k_hbm, keys), (v_hbm, vals)))
        ]

    for d in range(1, reach + 1):
        @pl.when(me + d < seqs)
        def _():
            for copy in kv_copies(d, me + d):
                copy.start()

    for d in range(1, reach + 1):
        @pl.when(me >= d)
        def _():
            for copy in kv_copies(d, me - d):
                copy.wait_recv()

    w_copy.start()
    at_end = (b == 0) | (b == n - 1)

    def part_send(source, index, here, there, sem, cols):
        slot = lax.rem(head - source - 1 + 2 * groups, groups)

        @pl.when(head != source)
        def _():
            pltpu.make_async_remote_copy(
                src_ref=stage.at[index, here, cols],
                dst_ref=incoming.at[slot, there, cols],
                send_sem=c_send.at[source], recv_sem=c_recv.at[slot, sem],
                device_id={"heads": source}, device_id_type=MESH,
            ).start()

    def over_tiles(body, width=COLS):
        def tile(t, _):
            body(pl.ds(pl.multiple_of(t * width, width), width))
            return 0

        lax.fori_loop(0, columns // width, tile, 0)

    def product(lhs, depth, cols):
        return jnp.dot(lhs, w_ref[depth, cols], preferred_element_type=jnp.float32)

    def project_pair(index):
        for source in range(n):
            @pl.when(at_end & (source != b))
            def _():
                z_wait(source, 2 * index, 2 * index, every)
                z_wait(source, 2 * index + 1, 2 * index + 1, every)

        def body(cols):
            stage[index, :, cols] = product(gath[index], every, cols).astype(jnp.bfloat16)
            for source in range(n):
                spot = pl.ds(source * pair, pair)
                part_send(source, index, spot, pair_rows(index), index, cols)

        over_tiles(body)

    half = PIECES // 2 - 1

    def spots(piece):
        return [pl.ds(s * pair + (piece % 2) * rows, rows) for s in range(n)]

    def project_one():
        piece = last - 1
        for source in range(n):
            @pl.when(at_end & (source != b))
            def _():
                z_wait(source, piece, piece, every)

        def body(cols):
            lhs = jnp.concatenate([gath[half, spot, :] for spot in spots(piece)], axis=0)
            part = product(lhs, every, cols).astype(jnp.bfloat16)
            for source, spot in enumerate(spots(piece)):
                stage[half, spot, cols] = part[source * rows:(source + 1) * rows]
                part_send(source, half, spot, pl.ds(piece * rows, rows), half, cols)

        over_tiles(body)

    def project_last():
        for part in range(PARTS):
            for source in range(n):
                @pl.when(at_end & (source != b))
                def _():
                    z_wait(source, last, last + part, part_cols(part))

            def body(cols):
                lhs = jnp.concatenate(
                    [gath[half, spot, part_cols(part)] for spot in spots(last)], axis=0
                )
                total = product(lhs, part_cols(part), cols)
                if part > 0:
                    total = total + acc[:, cols]
                if part < PARTS - 1:
                    acc[:, cols] = total
                    return
                total = total.astype(jnp.bfloat16)
                for source, spot in enumerate(spots(last)):
                    stage[half, spot, cols] = total[source * rows:(source + 1) * rows]
                    part_send(source, half, spot, pl.ds(last * rows, rows), half + 1, cols)

            over_tiles(body, COLS if part == PARTS - 1 else 2 * COLS)

    def collect(index, here, there, sem):
        for slot in range(groups - 1):
            spot = incoming.at[slot, there]
            pltpu.make_async_copy(spot, spot, c_recv.at[slot, sem]).wait()

        def body(cols):
            total = stage[index, here, cols].astype(jnp.float32)
            for slot in range(groups - 1):
                total = total + incoming[slot, there, cols].astype(jnp.float32)
            out_ref[0, there, cols] = total.astype(jnp.bfloat16)

        over_tiles(body)

    def collect_one(piece, sem):
        collect(*place(head, piece), piece_rows(piece), sem)

    behind = (n - 1) * HOP
    hold = (n - 2) * HOP

    def step(i, _):
        @pl.when(i < PIECES)
        def _():
            @pl.when(i == 1)
            def _():
                loads[4].wait()

            @pl.when((i > 0) | (me > 0))
            def _():
                attend(i)

        for way in range(2):
            late = b == (n - 2 if way == 0 else 1)
            for d in range(n - 1):
                source = b - d if way == 0 else b + d
                begin = hold + sum(hold - e * HOP for e in range(d))
                early = i - d * HOP
                kept = i - hold
                move(
                    way, source, early,
                    jnp.logical_not(late) | (i < begin) | (d == n - 2), d == 0,
                )
                if d < n - 2:
                    move(
                        way, source, kept,
                        late & (kept >= begin - d * HOP) & (kept < last), d == 0,
                    )

            @pl.when(late & (i == last + hold))
            def _():
                for part in range(PARTS):
                    for d in range(n - 1):
                        source = b - d if way == 0 else b + d
                        if d > 0:
                            z_wait(source, last, last + part, part_cols(part))
                        z_copy(way, source, last, last + part, part_cols(part)).start()

        @pl.when(i == behind)
        def _():
            w_copy.wait()

        r = i - behind
        odd = lax.rem(jnp.maximum(r, 0), 2) == 1
        index = lax.div(jnp.maximum(r, 0), 2)

        @pl.when(odd & (r < last))
        def _():
            project_pair(index)

        @pl.when(r == last - 1)
        def _():
            project_one()

        @pl.when(r == last)
        def _():
            project_last()

        @pl.when(odd & (r >= 3) & (r <= last))
        def _():
            collect(index - 1, pair_rows(head), pair_rows(index - 1), index - 1)

        return 0

    lax.fori_loop(0, behind + PIECES, step, 0)
    collect_one(last - 1, half)
    collect_one(last, half + 1)

    for d in range(1, reach + 1):
        @pl.when(me + d < seqs)
        def _():
            for copy in kv_copies(d, me + d):
                copy.wait_send()

    def drain(like, sem):
        pltpu.make_async_copy(like, like, sem).wait()

    for source in range(n):
        for way in range(2):
            @pl.when(goes(way, source))
            def _():
                drain(queries, z_send.at[way, source])

        @pl.when(head != source)
        def _():
            drain(out_ref.at[0], c_send.at[source])


def solution(mesh):
    seqs, groups, n = mesh.shape["seq"], mesh.shape["heads"], mesh.shape["batch"]

    def per_device(queries, keys, values, doc_lengths, out_weight):
        shard_len, q_width = queries.shape[1:]
        kv_width = keys.shape[2]
        columns = out_weight.shape[1]
        seq_total = seqs * shard_len
        longest = seq_total // 2 + shard_len // 2
        reach = min((longest + shard_len - 2) // shard_len, seqs - 1)
        rows = shard_len // PIECES
        pairs = PIECES // 2
        key_count = (reach + 1) * shard_len
        hbm = pl.BlockSpec(memory_space=pltpu.HBM)
        dma = pltpu.SemaphoreType.DMA
        return pl.pallas_call(
            functools.partial(kernel, (seqs, groups, n, reach)),
            out_shape=pltpu.VMEM((1, shard_len, columns), jnp.bfloat16),
            in_specs=[hbm] * 5,
            out_specs=pl.BlockSpec(memory_space=pltpu.VMEM),
            scratch_shapes=[
                pltpu.VMEM(out_weight.shape, jnp.bfloat16),
                pltpu.VMEM((shard_len, q_width), jnp.bfloat16),
                pltpu.VMEM((key_count, kv_width), jnp.bfloat16),
                pltpu.VMEM((key_count, kv_width), jnp.bfloat16),
                pltpu.SMEM(doc_lengths.shape, jnp.int32),
                pltpu.VMEM((pairs, 2 * n * rows, q_width), jnp.bfloat16),
                pltpu.VMEM((pairs, 2 * n * rows, columns), jnp.bfloat16),
                pltpu.VMEM((groups - 1, shard_len, columns), jnp.bfloat16),
                pltpu.VMEM((n * rows, columns), jnp.float32),
                dma,
                dma((5,)),
                dma((2, max(reach, 1))),
                dma((2, max(reach, 1))),
                dma((2, n)),
                dma((n, PIECES - 1 + PARTS)),
                dma((n,)),
                dma((groups - 1, pairs + 1)),
            ],
            compiler_params=pltpu.CompilerParams(
                collective_id=0, has_side_effects=True, vmem_limit_bytes=48 * 2**20
            ),
        )(*(
            pltpu.with_memory_space_constraint(x, pltpu.HBM)
            for x in (queries, keys, values, doc_lengths, out_weight)
        ))

    return jax.shard_map(
        per_device,
        mesh=mesh,
        in_specs=(
            P("batch", "seq", "heads"),
            P("batch", "seq", "heads"),
            P("batch", "seq", "heads"),
            P("batch", None),
            P("heads", "batch"),
        ),
        out_specs=P("heads", "seq", "batch"),
        check_vma=False,
    )
```
